256 devices in a mesh: batch: 8 (over y, core), pts: 32 (over z, x).
Axes of the slice: x: 4, y: 4, z: 8, core: 2. Of those that a mesh axis runs over, the one named last changes fastest.
Arguments:
- mesh_attributes: bfloat16 [262144, 512], P(('batch', 'pts')), parts along dimension 0, may hold values from -12 to 12
- occupied_vertices_tally: int32 [256], P(('batch', 'pts')), parts along dimension 0, may hold values from 512 to 1024, as said below
- vertex_content_matrix: bfloat16 [4, 512, 512], replicated, may hold values from -0.25 to 0.25
- vertex_partition_matrix: bfloat16 [4, 512, 512], replicated, may hold values from -0.25 to 0.25
- partition_affinity_matrix: bfloat16 [4, 8, 64, 64], replicated, may hold values from -0.75 to 0.75
- softmax_sharpness: float32 [4, 8], replicated, may hold values from 0.02 to 1
- partition_asking_matrix: bfloat16 [4, 64, 64], replicated, may hold values from -0.75 to 0.75
- partition_matching_matrix: bfloat16 [4, 64, 64], replicated, may hold values from -0.75 to 0.75
- partition_content_matrix: bfloat16 [4, 64, 64], replicated, may hold values from -0.75 to 0.75
- attention_result_matrix: bfloat16 [4, 512, 512], replicated, may hold values from -0.25 to 0.25
- widening_matrix: bfloat16 [4, 512, 512], replicated, may hold values from -0.25 to 0.25
- contracting_matrix: bfloat16 [4, 512, 512], replicated, may hold values from -0.25 to 0.25
Outputs:
- result: bfloat16 [262144, 512], P(('batch', 'pts')), parts along dimension 0
The draws below stay inside these ranges and needn't reach their ends.
There are 8 independent parts, one for each index of `batch`. The reference program is written for one: setup_inputs(seed, part) draws one part's arguments, and reference() takes and returns one part's arrays. A program takes and returns all parts, laid end to end along the dimension named above; an argument that names none is the same for every part. Nothing has to cross between parts.
Inputs may be any that keep to these rules, and one draw needn't show every extreme that they name: `occupied_vertices_tally`: the shard of some index holds 1024 live points in every draw.
All inputs are finite; a program needn't handle non-finite values.
Results may differ from the reference program's by a relative error of at most 0.0055.
Values sent between devices are 32-bit elements; how exact they have to be, the bound alone decides.
No kernel may reach another device: no remote copies, remote signals or barrier semaphores. Data moves between devices by JAX's collectives and lax.ppermute only.
A program may use at most 64 MiB of HBM per device.

```python
import jax
import jax.numpy as jnp
from jax import lax

D = 512
H = 8
DH = 64
G = 64
FF = 512
LAYERS = 4
PTS_DEV = 1024
POINTS = 32768
N_PTS = 32


def draw_mesh_attributes(key, part):
    keys = jax.random.split(jax.random.fold_in(key, 11), 5)
    position = jnp.arange(POINTS, dtype=jnp.float32) / POINTS
    freqs = jnp.arange(1, 5, dtype=jnp.float32)
    phase = jax.random.uniform(keys[0], (4,), minval=0.0, maxval=6.2831853)
    basis = jnp.sin(6.2831853 * position[:, None] * freqs[None, :] + phase[None, :])
    direction = jax.random.normal(keys[1], (4, D), dtype=jnp.float32)
    smooth = jnp.dot(basis, direction, precision=lax.Precision.HIGHEST)
    regional = jnp.repeat(3.0 * jax.random.normal(keys[4], (N_PTS, D), dtype=jnp.float32), PTS_DEV, axis=0)
    field = jax.random.normal(keys[2], (POINTS, D), dtype=jnp.float32) + smooth + regional
    return jnp.clip(field, -12.0, 12.0).astype(jnp.bfloat16)


def draw_occupied_vertices_tally(key, part):
    keys = jax.random.split(jax.random.fold_in(key, 23), 2)
    drawn = jax.random.randint(keys[0], (N_PTS,), PTS_DEV // 2, PTS_DEV + 1)
    filled = jax.random.randint(keys[1], (), 0, N_PTS)
    return jnp.where(jnp.arange(N_PTS) == filled, PTS_DEV, drawn).astype(jnp.int32)


def draw_softmax_sharpness(key, part):
    lowest = 0.12
    uniform_draw = jax.random.uniform(jax.random.fold_in(key, 37), (LAYERS, H), dtype=jnp.float32)
    return jnp.exp(jnp.log(lowest) * (1.0 - uniform_draw))


def bell_draw(stream_key, extent, width, most, kind=jnp.bfloat16):
    result = jax.random.normal(stream_key, extent, jnp.float32) * width
    return jnp.minimum(jnp.maximum(result, -most), most).astype(kind)


def setup_inputs(seed: int = 0, part: int = 0) -> dict:
    seeds = jax.random.split(jax.random.key(seed), 13)
    own_keys = jax.random.split(jax.random.fold_in(seeds[12], part), 13)
    mesh_attributes = draw_mesh_attributes(jax.random.fold_in(jax.random.fold_in(seeds[12], part), 71), part)
    occupied_vertices_tally = draw_occupied_vertices_tally(jax.random.fold_in(jax.random.fold_in(seeds[12], part), 71), part)
    vertex_content_matrix = bell_draw(seeds[2], (LAYERS, D, D), D ** -0.5, 0.25)
    vertex_partition_matrix = bell_draw(seeds[3], (LAYERS, D, D), D ** -0.5, 0.25)
    partition_affinity_matrix = bell_draw(seeds[4], (LAYERS, H, DH, G), DH ** -0.5, 0.75)
    softmax_sharpness = draw_softmax_sharpness(jax.random.fold_in(seeds[12], 71), part)
    partition_asking_matrix = bell_draw(seeds[6], (LAYERS, DH, DH), DH ** -0.5, 0.75)
    partition_matching_matrix = bell_draw(seeds[7], (LAYERS, DH, DH), DH ** -0.5, 0.75)
    partition_content_matrix = bell_draw(seeds[8], (LAYERS, DH, DH), DH ** -0.5, 0.75)
    attention_result_matrix = bell_draw(seeds[9], (LAYERS, D, D), D ** -0.5, 0.25)
    widening_matrix = bell_draw(seeds[10], (LAYERS, D, FF), D ** -0.5, 0.25)
    contracting_matrix = bell_draw(seeds[11], (LAYERS, FF, D), FF ** -0.5, 0.25)
    return dict(mesh_attributes=mesh_attributes, occupied_vertices_tally=occupied_vertices_tally, vertex_content_matrix=vertex_content_matrix, vertex_partition_matrix=vertex_partition_matrix, partition_affinity_matrix=partition_affinity_matrix, softmax_sharpness=softmax_sharpness, partition_asking_matrix=partition_asking_matrix, partition_matching_matrix=partition_matching_matrix, partition_content_matrix=partition_content_matrix, attention_result_matrix=attention_result_matrix, widening_matrix=widening_matrix, contracting_matrix=contracting_matrix)


def layer_norm(stream):
    average = lax.optimization_barrier(jnp.mean(stream, axis=-1, keepdims=True))
    centred = stream - average
    variance = lax.optimization_barrier(jnp.mean(centred * centred, axis=-1, keepdims=True))
    return centred * lax.rsqrt(variance + 1e-05)

def attend_slices(tokens, partition_asking_matrix, partition_matching_matrix, partition_content_matrix):
    highest = lax.Precision.HIGHEST
    queries = jnp.einsum('hgd,de->hge', tokens, partition_asking_matrix.astype(jnp.float32), precision=highest)
    key_rows = jnp.einsum('hgd,de->hge', tokens, partition_matching_matrix.astype(jnp.float32), precision=highest)
    val_rows = jnp.einsum('hgd,de->hge', tokens, partition_content_matrix.astype(jnp.float32), precision=highest)
    scores = jnp.einsum('hgd,hkd->hgk', queries, key_rows, precision=highest) * queries.shape[-1] ** (-0.5)
    attn_probs = jax.nn.softmax(scores, axis=-1)
    return jnp.einsum('hgk,hkd->hgd', attn_probs, val_rows, precision=highest)

def reference(mesh_attributes, occupied_vertices_tally, vertex_content_matrix, vertex_partition_matrix, partition_affinity_matrix, softmax_sharpness, partition_asking_matrix, partition_matching_matrix, partition_content_matrix, attention_result_matrix, widening_matrix, contracting_matrix):
    points = mesh_attributes.shape[0]
    live = jnp.arange(PTS_DEV, dtype=jnp.int32)[None, :] < occupied_vertices_tally[:, None]
    live_mask = live.reshape(points).astype(jnp.float32)
    stream = mesh_attributes.astype(jnp.float32)
    for stacked_level_index in range(LAYERS):
        normed = layer_norm(stream).astype(jnp.bfloat16)
        values = jnp.dot(normed, vertex_content_matrix[stacked_level_index], preferred_element_type=jnp.float32).astype(jnp.bfloat16)
        slice_feats = jnp.dot(normed, vertex_partition_matrix[stacked_level_index], preferred_element_type=jnp.float32).astype(jnp.bfloat16)
        partition_raw_affinities = jnp.einsum('phd,hdg->phg', slice_feats.reshape(points, H, DH).astype(jnp.float32), partition_affinity_matrix[stacked_level_index].astype(jnp.float32))
        partition_raw_affinities = partition_raw_affinities / softmax_sharpness[stacked_level_index][None, :, None]
        weights = (jax.nn.softmax(partition_raw_affinities, axis=-1) * live_mask[:, None, None]).astype(jnp.bfloat16)
        numerator = jnp.einsum('phg,phd->hgd', weights.astype(jnp.float32), values.reshape(points, H, DH).astype(jnp.float32))
        mass = lax.optimization_barrier(jnp.sum(weights.astype(jnp.float32), axis=0))
        tokens = numerator / (mass + 1e-05)[:, :, None]
        attended = attend_slices(tokens, partition_asking_matrix[stacked_level_index], partition_matching_matrix[stacked_level_index], partition_content_matrix[stacked_level_index]).astype(jnp.bfloat16)
        spread = jnp.einsum('phg,hgd->phd', weights.astype(jnp.float32), attended.astype(jnp.float32))
        spread = spread.reshape(points, D).astype(jnp.bfloat16)
        stream = stream + jnp.dot(spread, attention_result_matrix[stacked_level_index], preferred_element_type=jnp.float32)
        normed = layer_norm(stream).astype(jnp.bfloat16)
        hidden = jax.nn.gelu(jnp.dot(normed, widening_matrix[stacked_level_index], preferred_element_type=jnp.float32)).astype(jnp.bfloat16)
        stream = stream + jnp.dot(hidden, contracting_matrix[stacked_level_index], preferred_element_type=jnp.float32)
    return (stream * live_mask[:, None]).astype(jnp.bfloat16)
```

```python
import functools
import jax
import jax.numpy as jnp
from jax import lax
from jax.experimental import pallas as pl
from jax.experimental.pallas import tpu as pltpu
from jax.sharding import PartitionSpec as P

F32 = jnp.float32
BF16 = jnp.bfloat16
TILE = 256
LOG2E = 1.4426950408889634
PAY_ROWS = 288


def dot(a, b, ca=1, cb=0):
    return lax.dot_general(a, b, (((ca,), (cb,)), ((), ())), preferred_element_type=F32)


def split2(x):
    hi = x.astype(BF16)
    lo = (x - hi.astype(F32)).astype(BF16)
    return hi, lo


def dot3(a, b, ca=1, cb=0):
    ah, al = split2(a)
    bh, bl = split2(b)
    return dot(ah, bh, ca, cb) + (dot(ah, bl, ca, cb) + dot(al, bh, ca, cb))


def layer_norm(x):
    c = x - jnp.mean(x, axis=-1, keepdims=True)
    v = jnp.mean(c * c, axis=-1, keepdims=True)
    return c * lax.rsqrt(v + 1e-05)


def same_block(rows, cols, size):
    r = lax.broadcasted_iota(jnp.int32, (rows, cols), 0) // size
    c = lax.broadcasted_iota(jnp.int32, (rows, cols), 1) // size
    return r == c


def pair_diag(w):
    w2 = jnp.concatenate([w, w], axis=1)
    w4 = jnp.concatenate([w2, w2], axis=0)
    return jnp.where(same_block(128, 128, 64), w4, jnp.zeros_like(w4))


def attend(agg, ask, match, content, res_ref, m_ref):
    left = lax.broadcasted_iota(jnp.int32, (64, 128), 1) < 64
    mass = agg[256:264, :].T
    rows = []
    for p in range(4):
        den = jnp.where(left, mass[0:64, p : p + 1], mass[64:128, p : p + 1]) + 1e-05
        rows.append(agg[64 * p : 64 * p + 64, :] / den)
    tokens = jnp.concatenate(rows, axis=0)
    maps = jnp.concatenate([pair_diag(ask), pair_diag(match), pair_diag(content)], axis=1)
    th, tl = split2(tokens)
    qkv = dot(th, maps) + dot(tl, maps)
    keep = same_block(128, 128, 64)
    for p in range(4):
        q = qkv[64 * p : 64 * p + 64, 0:128]
        k = qkv[64 * p : 64 * p + 64, 128:256]
        v = qkv[64 * p : 64 * p + 64, 256:384]
        zero = jnp.zeros_like(q)
        q2 = jnp.concatenate([jnp.where(left, q, zero), jnp.where(left, zero, q)], axis=0)
        scores = dot3(q2, k, 1, 1) * 0.125
        e = jnp.exp(scores - jnp.max(scores, axis=-1, keepdims=True))
        probs = e / jnp.sum(e, axis=-1, keepdims=True)
        att = dot3(probs, v)
        att = jnp.where(keep, att, jnp.zeros_like(att)).astype(BF16)
        m_ref[128 * p : 128 * p + 128, :] = dot(att, res_ref[128 * p : 128 * p + 128, :]).astype(BF16)


def affinity_t(aff, j):
    a = aff[4 * j : 4 * j + 4].reshape(256, 64)
    a4 = jnp.concatenate([a, a, a, a], axis=1)
    a4 = jnp.where(same_block(256, 256, 64), a4, jnp.zeros_like(a4))
    return a4.T


def slice_tile(s, t, tally, coef, v_w, pt_ref, aff_t, w_ref, y_ref, mass_ref):
    n = layer_norm(s).astype(BF16)
    values = dot(n, v_w).astype(BF16)
    ft = dot(pt_ref[...], n, 1, 1).astype(BF16)
    cols = lax.broadcasted_iota(jnp.int32, (1, TILE), 1) + t * TILE
    live = (cols < tally).astype(F32)
    for j in range(2):
        logits = dot(aff_t[j], ft[256 * j : 256 * j + 256, :])
        for i in range(4):
            h = 4 * j + i
            lg = logits[64 * i : 64 * i + 64, :]
            e = jnp.exp2((lg - jnp.max(lg, axis=0, keepdims=True)) * coef[h])
            r = live / jnp.sum(e, axis=0, keepdims=True)
            w = (e * r).astype(BF16)
            w_ref[64 * h : 64 * h + 64, TILE * t : TILE * t + TILE] = w
            wf = w.astype(F32)
            part = wf[:, 0:128]
            for q in range(1, TILE // 128):
                part = part + wf[:, 128 * q : 128 * q + 128]
            if t == 0:
                mass_ref[64 * h : 64 * h + 64, :] = part
            else:
                mass_ref[64 * h : 64 * h + 64, :] += part
        y = dot(
            w_ref[256 * j : 256 * j + 256, TILE * t : TILE * t + TILE],
            values[:, 256 * j : 256 * j + 256],
        )
        if t == 0:
            y_ref[j] = y
        else:
            y_ref[j] += y


def payload(y_ref, mass_ref, pay_ref):
    left = lax.broadcasted_iota(jnp.int32, (64, 128), 1) < 64
    for p in range(4):
        j, q = p // 2, p % 2
        even = y_ref[j, 128 * q : 128 * q + 64, 128 * q : 128 * q + 128]
        odd = y_ref[j, 128 * q + 64 : 128 * q + 128, 128 * q : 128 * q + 128]
        pay_ref[64 * p : 64 * p + 64, :] = jnp.where(left, even, odd)
        row = jnp.sum(mass_ref[128 * p : 128 * p + 128, :].T, axis=0, keepdims=True)
        pay_ref[256 + p : 257 + p, :] = row
    pay_ref[260:PAY_ROWS, :] = jnp.zeros((PAY_ROWS - 260, 128), F32)


def boundary_kernel(layer, first, last, points, *refs):
    refs = list(refs)
    tally_ref, sharp_ref = refs.pop(0), refs.pop(0)
    if not first:
        agg_ref = refs.pop(0)
    s_ref = refs.pop(0)
    if not first:
        w_in_ref = refs.pop(0)
        ask_h, match_h, content_h, res_h, wide_h, narrow_h = refs[:6]
        refs = refs[6:]
    if not last:
        val_h, part_h, aff_h = refs[:3]
        refs = refs[3:]
    if last:
        out_ref = refs.pop(0)
    else:
        if not first:
            s_out_ref = refs.pop(0)
        w_ref, pay_ref = refs.pop(0), refs.pop(0)
    copies = {}

    def fetch(name, src, dst, sem):
        copy = pltpu.make_async_copy(src, dst, sem)
        copy.start()
        copies[name] = copy

    if not first:
        ask_v, match_v, content_v, res_v, wide_v, narrow_v, m_ref, sems_a = refs[:8]
        refs = refs[8:]
        for i, (n, a, b) in enumerate(
            [
                ("ask", ask_h, ask_v),
                ("match", match_h, match_v),
                ("content", content_h, content_v),
                ("res", res_h, res_v),
                ("wide", wide_h, wide_v),
                ("narrow", narrow_h, narrow_v),
            ]
        ):
            fetch(n, a.at[layer - 1], b, sems_a.at[i])
    if not last:
        val_v, part_v, aff_v, pt_ref, y_ref, mass_ref, sems_b = refs
        for i, (n, a, b) in enumerate(
            [("part", part_h, part_v), ("aff", aff_h, aff_v), ("val", val_h, val_v)]
        ):
            fetch(n, a.at[layer], b, sems_b.at[i])
    tally = tally_ref[0]

    if not first:
        for n in ("ask", "match", "content", "res"):
            copies[n].wait()
        attend(agg_ref, ask_v[...], match_v[...], content_v[...], res_v, m_ref)
    if not last:
        copies["part"].wait()
        copies["aff"].wait()
        pt_ref[...] = part_v[...].T
        aff_t = [affinity_t(aff_v[...], 0), affinity_t(aff_v[...], 1)]
        coef = [LOG2E / sharp_ref[layer : layer + 1, h : h + 1] for h in range(8)]
        copies["val"].wait()
    if not first:
        copies["wide"].wait()
        copies["narrow"].wait()

    for t in range(points // TILE):
        at = slice(t * TILE, t * TILE + TILE)
        s = s_ref[at, :].astype(F32)
        if not first:
            s = s + dot(w_in_ref[:, at], m_ref[...], 0, 0)
            n = layer_norm(s).astype(BF16)
            hidden = jax.nn.gelu(dot(n, wide_v[...])).astype(BF16)
            s = s + dot(hidden, narrow_v[...])
        if last:
            rows = lax.broadcasted_iota(jnp.int32, (TILE, 1), 0) + t * TILE
            out_ref[at, :] = jnp.where(rows < tally, s, jnp.zeros_like(s)).astype(BF16)
        else:
            if not first:
                s_out_ref[at, :] = s
            slice_tile(s, t, tally, coef, val_v[...], pt_ref, aff_t, w_ref, y_ref, mass_ref)
    if not last:
        payload(y_ref, mass_ref, pay_ref)


def boundary(layer, layers, tally, sharp, agg, s, w, mats):
    first, last = layer == 0, layer == layers
    points, dim = s.shape
    ask, match, content, res, wide, narrow, val, part, aff = mats
    vmem = pl.BlockSpec(memory_space=pltpu.VMEM)
    smem = pl.BlockSpec(memory_space=pltpu.SMEM)
    hbm = pl.BlockSpec(memory_space=pltpu.HBM)
    args, specs = [tally, sharp], [smem, vmem]
    scratch = []
    sq = (dim, dim)
    if not first:
        args += [agg]
        specs += [vmem]
    args += [s]
    specs += [vmem]
    if not first:
        args += [w, ask, match, content, res, wide, narrow]
        specs += [vmem] + [hbm] * 6
        scratch += [pltpu.VMEM((64, 64), BF16)] * 3 + [pltpu.VMEM(sq, BF16)] * 4
        scratch += [pltpu.SemaphoreType.DMA((6,))]
    if not last:
        args += [val, part, aff]
        specs += [hbm] * 3
        scratch += [
            pltpu.VMEM(sq, BF16),
            pltpu.VMEM(sq, BF16),
            pltpu.VMEM((8, 64, 64), BF16),
            pltpu.VMEM(sq, BF16),
            pltpu.VMEM((2, 256, 256), F32),
            pltpu.VMEM((512, 128), F32),
            pltpu.SemaphoreType.DMA((3,)),
        ]
    if last:
        outs = [jax.ShapeDtypeStruct((points, dim), BF16)]
    else:
        outs = [] if first else [pltpu.VMEM((points, dim), F32)]
        outs += [pltpu.VMEM((dim, points), BF16), pltpu.VMEM((PAY_ROWS, 128), F32)]
    return pl.pallas_call(
        functools.partial(boundary_kernel, layer, first, last, points),
        out_shape=outs,
        in_specs=specs,
        out_specs=[vmem] * len(outs),
        scratch_shapes=scratch,
        compiler_params=pltpu.CompilerParams(vmem_limit_bytes=24 * 1024 * 1024),
        name=f"boundary{layer}",
    )(*args)


def fold_kernel(peers, got_ref, out_ref):
    step = PAY_ROWS // peers
    for r in range(step):
        rows = pl.ds(r, peers, stride=step)
        total = jnp.sum(got_ref[rows, :], axis=0, keepdims=True)
        out_ref[rows, :] = jnp.broadcast_to(total, (peers, 128))


def summed(pay):
    peers = lax.axis_size("pts")
    got = lax.all_to_all(pay.reshape(peers, 1, -1), "pts", 0, 0, tiled=True)
    vmem = pl.BlockSpec(memory_space=pltpu.VMEM)
    own = pl.pallas_call(
        functools.partial(fold_kernel, peers),
        out_shape=pltpu.VMEM((PAY_ROWS, 128), F32),
        in_specs=[vmem],
        out_specs=vmem,
        compiler_params=pltpu.CompilerParams(vmem_limit_bytes=2 * 1024 * 1024),
        name="fold",
    )(got.reshape(PAY_ROWS, 128))
    every = lax.all_to_all(own.reshape(peers, 1, -1), "pts", 0, 0, tiled=True)
    return every.reshape(PAY_ROWS, 128)


def per_device(x, tally, val, part, aff, sharp, ask, match, content, res, wide, narrow):
    mats = (ask, match, content, res, wide, narrow, val, part, aff)
    mats = [pltpu.with_memory_space_constraint(m, pltpu.HBM) for m in mats]
    layers = val.shape[0]
    w, pay = boundary(0, layers, tally, sharp, None, x, None, mats)
    s = x
    for layer in range(1, layers + 1):
        agg = summed(pay)
        got = boundary(layer, layers, tally, sharp, agg, s, w, mats)
        if layer < layers:
            s, w, pay = got
    return got[0]


def solution(mesh):
    placed = (P(("batch", "pts"), None), P(("batch", "pts"))) + (P(),) * 10
    return jax.shard_map(
        per_device, mesh=mesh, in_specs=placed, out_specs=P(("batch", "pts"), None), check_vma=False
    )
```

```python
import functools
import jax
import jax.numpy as jnp
from jax import lax
from jax.experimental import pallas as pl
from jax.experimental.pallas import tpu as pltpu
from jax.sharding import PartitionSpec as P

F32 = jnp.float32
BF16 = jnp.bfloat16
TILE = 1024
LOG2E = 1.4426950408889634
PAY_ROWS = 288
VMEM_LIMIT = 16 * 1024 * 1024


def dot(a, b, ca=1, cb=0):
    return lax.dot_general(a, b, (((ca,), (cb,)), ((), ())), preferred_element_type=F32)


def split2(x):
    hi = x.astype(BF16)
    lo = (x - hi.astype(F32)).astype(BF16)
    return hi, lo


def dot3(a, b, ca=1, cb=0):
    ah, al = split2(a)
    bh, bl = split2(b)
    return dot(ah, bh, ca, cb) + (dot(ah, bl, ca, cb) + dot(al, bh, ca, cb))


def layer_norm(x):
    c = x - jnp.mean(x, axis=-1, keepdims=True)
    v = jnp.mean(c * c, axis=-1, keepdims=True)
    return c * lax.rsqrt(v + 1e-05)


def same_block(rows, cols, size):
    r = lax.broadcasted_iota(jnp.int32, (rows, cols), 0) // size
    c = lax.broadcasted_iota(jnp.int32, (rows, cols), 1) // size
    return r == c


def pair_diag(w):
    w2 = jnp.concatenate([w, w], axis=1)
    w4 = jnp.concatenate([w2, w2], axis=0)
    return jnp.where(same_block(128, 128, 64), w4, jnp.zeros_like(w4))


def attend(agg, ask, match, content, res_ref, m_ref):
    left = lax.broadcasted_iota(jnp.int32, (64, 128), 1) < 64
    mass = agg[256:264, :].T
    rows = []
    for p in range(4):
        den = jnp.where(left, mass[0:64, p : p + 1], mass[64:128, p : p + 1]) + 1e-05
        rows.append(agg[64 * p : 64 * p + 64, :] / den)
    tokens = jnp.concatenate(rows, axis=0)
    maps = jnp.concatenate([pair_diag(ask), pair_diag(match), pair_diag(content)], axis=1)
    th, tl = split2(tokens)
    qkv = dot(th, maps) + dot(tl, maps)
    keep = same_block(128, 128, 64)
    for p in range(4):
        q = qkv[64 * p : 64 * p + 64, 0:128]
        k = qkv[64 * p : 64 * p + 64, 128:256]
        v = qkv[64 * p : 64 * p + 64, 256:384]
        zero = jnp.zeros_like(q)
        q2 = jnp.concatenate([jnp.where(left, q, zero), jnp.where(left, zero, q)], axis=0)
        scores = dot3(q2, k, 1, 1) * 0.125
        e = jnp.exp(scores - jnp.max(scores, axis=-1, keepdims=True))
        probs = e / jnp.sum(e, axis=-1, keepdims=True)
        att = dot3(probs, v)
        att = jnp.where(keep, att, jnp.zeros_like(att)).astype(BF16)
        m_ref[128 * p : 128 * p + 128, :] = dot(att, res_ref[128 * p : 128 * p + 128, :]).astype(BF16)


def affinity_t(aff, j):
    a = aff[4 * j : 4 * j + 4].reshape(256, 64)
    a4 = jnp.concatenate([a, a, a, a], axis=1)
    a4 = jnp.where(same_block(256, 256, 64), a4, jnp.zeros_like(a4))
    return a4.T


def slice_tile(s, t, tally, coef, v_w, pt_ref, aff_t, w_ref, y_ref, mass_ref):
    n = layer_norm(s).astype(BF16)
    values = dot(n, v_w).astype(BF16)
    ft = dot(pt_ref[...], n, 1, 1).astype(BF16)
    cols = lax.broadcasted_iota(jnp.int32, (1, TILE), 1) + t * TILE
    live = (cols < tally).astype(F32)
    for j in range(2):
        logits = dot(aff_t[j], ft[256 * j : 256 * j + 256, :])
        for i in range(4):
            h = 4 * j + i
            lg = logits[64 * i : 64 * i + 64, :]
            e = jnp.exp2((lg - jnp.max(lg, axis=0, keepdims=True)) * coef[h])
            r = live / jnp.sum(e, axis=0, keepdims=True)
            w = (e * r).astype(BF16)
            w_ref[t, 64 * h : 64 * h + 64, :] = w
            wf = w.astype(F32)
            part = wf[:, 0:128]
            for q in range(1, TILE // 128):
                part = part + wf[:, 128 * q : 128 * q + 128]
            mass_ref[64 * h : 64 * h + 64, :] += part
        y_ref[j] += dot(w_ref[t, 256 * j : 256 * j + 256, :], values[:, 256 * j : 256 * j + 256])


def payload(y_ref, mass_ref, pay_ref):
    left = lax.broadcasted_iota(jnp.int32, (64, 128), 1) < 64
    for p in range(4):
        j, q = p // 2, p % 2
        even = y_ref[j, 128 * q : 128 * q + 64, 128 * q : 128 * q + 128]
        odd = y_ref[j, 128 * q + 64 : 128 * q + 128, 128 * q : 128 * q + 128]
        pay_ref[64 * p : 64 * p + 64, :] = jnp.where(left, even, odd)
        row = jnp.sum(mass_ref[128 * p : 128 * p + 128, :].T, axis=0, keepdims=True)
        pay_ref[256 + p : 257 + p, :] = row
    pay_ref[260:PAY_ROWS, :] = jnp.zeros((PAY_ROWS - 260, 128), F32)


def boundary_kernel(layer, first, last, points, *refs):
    refs = list(refs)
    tally_ref = refs.pop(0)
    tally = tally_ref[0]
    tiles = points // TILE
    if first:
        sharp_h, x_h, val_h, part_h, aff_h, wide_h, narrow_h = refs[:7]
        sharp_ref, s_ref, aff_ref, wide_ref, narrow_ref, w_ref, pay_ref = refs[7:14]
        val_ref, part_ref, pt_ref, y_ref, mass_ref, sems = refs[14:]
        pairs = [
            (x_h, s_ref),
            (part_h.at[layer], part_ref),
            (aff_h, aff_ref),
            (sharp_h, sharp_ref),
            (val_h.at[layer], val_ref),
            (wide_h, wide_ref),
            (narrow_h, narrow_ref),
        ]
        copies = [pltpu.make_async_copy(a, b, sems.at[i]) for i, (a, b) in enumerate(pairs)]
        for c in copies[:5]:
            c.start()
        for c in copies[:5]:
            c.wait()
        for c in copies[5:]:
            c.start()
        val_at = part_at = ()
        aff_at = (layer,)
    else:
        agg_ref, s_ref, w_in_ref, ask, match, content, res, wide, narrow = refs[:9]
        refs = refs[9:]
        if last:
            out_h, m_ref, out_ref, sems = refs
        else:
            sharp_ref, val_ref, part_ref, aff_ref, s_out_ref, w_ref, pay_ref = refs[:7]
            m_ref, pt_ref, y_ref, mass_ref = refs[7:]
            val_at = part_at = aff_at = (layer,)
    if not last:
        pt_ref[...] = part_ref[part_at + (slice(None), slice(None))].T
        aff = aff_ref[aff_at + (slice(None), slice(None), slice(None))]
        aff_t = [affinity_t(aff, 0), affinity_t(aff, 1)]
        coef = [LOG2E / sharp_ref[layer : layer + 1, h : h + 1] for h in range(8)]
        y_ref[...] = jnp.zeros_like(y_ref)
        mass_ref[...] = jnp.zeros_like(mass_ref)
    if not first:
        own = layer - 1
        attend(agg_ref, ask[own], match[own], content[own], res.at[own], m_ref)

    for t in range(tiles):
        at = slice(t * TILE, t * TILE + TILE)
        s = s_ref[at, :].astype(F32)
        if not first:
            s = s + dot(w_in_ref[t], m_ref[...], 0, 0)
            n = layer_norm(s).astype(BF16)
            hidden = jax.nn.gelu(dot(n, wide[own])).astype(BF16)
            s = s + dot(hidden, narrow[own])
        if last:
            rows = lax.broadcasted_iota(jnp.int32, (TILE, 1), 0) + t * TILE
            out_ref[at, :] = jnp.where(rows < tally, s, jnp.zeros_like(s)).astype(BF16)
            pltpu.make_async_copy(out_ref.at[at], out_h.at[at], sems.at[t]).start()
        else:
            if not first:
                s_out_ref[at, :] = s
            val = val_ref[val_at + (slice(None), slice(None))]
            slice_tile(s, t, tally, coef, val, pt_ref, aff_t, w_ref, y_ref, mass_ref)
    if last:
        for t in range(tiles):
            at = slice(t * TILE, t * TILE + TILE)
            pltpu.make_async_copy(out_ref.at[at], out_h.at[at], sems.at[t]).wait()
    else:
        payload(y_ref, mass_ref, pay_ref)
    if first:
        for c in copies[5:]:
            c.wait()


def boundary(layer, layers, tally, sharp, agg, s, w, mats):
    first, last = layer == 0, layer == layers
    points, dim = s.shape
    ask, match, content, res, wide, narrow, val, part, aff = mats
    vmem = pl.BlockSpec(memory_space=pltpu.VMEM)
    smem = pl.BlockSpec(memory_space=pltpu.SMEM)
    hbm = pl.BlockSpec(memory_space=pltpu.HBM)
    args, specs = [tally], [smem]
    scratch = []
    sq = (dim, dim)
    sums = [pltpu.VMEM(sq, BF16), pltpu.VMEM((2, 256, 256), F32), pltpu.VMEM((512, 128), F32)]
    if first:
        args += [sharp, s, val, part, aff, wide, narrow]
        specs += [hbm] * 7
        scratch += [pltpu.VMEM(sq, BF16), pltpu.VMEM(sq, BF16)]
        scratch += sums + [pltpu.SemaphoreType.DMA((7,))]
    else:
        args += [agg, s, w, ask, match, content, res, wide, narrow]
        specs += [vmem] * 9
        scratch += [pltpu.VMEM(sq, BF16)]
        if last:
            scratch += [pltpu.VMEM(s.shape, BF16), pltpu.SemaphoreType.DMA((points // TILE,))]
        else:
            args += [sharp, val, part, aff]
            specs += [vmem] * 4
            scratch += sums
    if last:
        outs = [jax.ShapeDtypeStruct((points, dim), BF16)]
    else:
        outs = [] if first else [pltpu.VMEM((points, dim), F32)]
        if first:
            outs = [pltpu.VMEM(m.shape, m.dtype) for m in (sharp, s, aff, wide, narrow)]
        outs += [pltpu.VMEM((points // TILE, dim, TILE), BF16), pltpu.VMEM((PAY_ROWS, 128), F32)]
    return pl.pallas_call(
        functools.partial(boundary_kernel, layer, first, last, points),
        out_shape=outs,
        in_specs=specs,
        out_specs=[hbm if last else vmem] * len(outs),
        scratch_shapes=scratch,
        compiler_params=pltpu.CompilerParams(vmem_limit_bytes=VMEM_LIMIT),
        name=f"boundary{layer}",
    )(*args)


def fold_kernel(peers, got_ref, out_ref):
    step = PAY_ROWS // peers
    for r in range(step):
        rows = pl.ds(r, peers, stride=step)
        total = jnp.sum(got_ref[rows, :], axis=0, keepdims=True)
        out_ref[rows, :] = jnp.broadcast_to(total, (peers, 128))


def summed(pay):
    peers = lax.axis_size("pts")
    got = lax.all_to_all(pay.reshape(peers, 1, -1), "pts", 0, 0, tiled=True)
    vmem = pl.BlockSpec(memory_space=pltpu.VMEM)
    own = pl.pallas_call(
        functools.partial(fold_kernel, peers),
        out_shape=pltpu.VMEM((PAY_ROWS, 128), F32),
        in_specs=[vmem],
        out_specs=vmem,
        compiler_params=pltpu.CompilerParams(vmem_limit_bytes=2 * 1024 * 1024),
        name="fold",
    )(got.reshape(PAY_ROWS, 128))
    every = lax.all_to_all(own.reshape(peers, 1, -1), "pts", 0, 0, tiled=True)
    return every.reshape(PAY_ROWS, 128)


def per_device(x, tally, val, part, aff, sharp, ask, match, content, res, wide, narrow):
    def placed(space, *arrays):
        return [pltpu.with_memory_space_constraint(a, space) for a in arrays]

    layers = val.shape[0]
    x, sharp, *far = placed(pltpu.HBM, x, sharp, val, part, aff, wide, narrow)
    far = [None] * 4 + [far[3], far[4], *far[:3]]
    sharp, s, aff, wide, narrow, w, pay = boundary(0, layers, tally, sharp, None, x, None, far)
    near = placed(pltpu.VMEM, ask, match, content, res) + [wide, narrow]
    near += placed(pltpu.VMEM, val, part) + [aff]
    for layer in range(1, layers + 1):
        got = boundary(layer, layers, tally, sharp, summed(pay), s, w, near)
        if layer < layers:
            s, w, pay = got
    return got[0]


def solution(mesh):
    placed = (P(("batch", "pts"), None), P(("batch", "pts"))) + (P(),) * 10
    return jax.shard_map(
        per_device, mesh=mesh, in_specs=placed, out_specs=P(("batch", "pts"), None), check_vma=False
    )
```

```python
import functools
import jax
import jax.numpy as jnp
from jax import lax
from jax.experimental import pallas as pl
from jax.experimental.pallas import tpu as pltpu
from jax.sharding import PartitionSpec as P

F32 = jnp.float32
BF16 = jnp.bfloat16
SLAB = 256
TILES = (1024, 512, 512)
LAG = 1
LOG2E = 1.4426950408889634
PAY_ROWS = 288
VMEM_LIMIT = 16 * 1024 * 1024


def dot(a, b, ca=1, cb=0):
    return lax.dot_general(a, b, (((ca,), (cb,)), ((), ())), preferred_element_type=F32)


def split2(x):
    hi = x.astype(BF16)
    lo = (x - hi.astype(F32)).astype(BF16)
    return hi, lo


def dot3(a, b, ca=1, cb=0):
    ah, al = split2(a)
    bh, bl = split2(b)
    return dot(ah, bh, ca, cb) + (dot(ah, bl, ca, cb) + dot(al, bh, ca, cb))


def layer_norm(x):
    c = x - jnp.mean(x, axis=-1, keepdims=True)
    v = jnp.mean(c * c, axis=-1, keepdims=True)
    return c * lax.rsqrt(v + 1e-05)


def same_block(rows, cols, size):
    r = lax.broadcasted_iota(jnp.int32, (rows, cols), 0) // size
    c = lax.broadcasted_iota(jnp.int32, (rows, cols), 1) // size
    return r == c


def pair_diag(w):
    w2 = jnp.concatenate([w, w], axis=1)
    w4 = jnp.concatenate([w2, w2], axis=0)
    return jnp.where(same_block(128, 128, 64), w4, jnp.zeros_like(w4))


def attend(agg, ask, match, content, res_ref, m_ref):
    keep = same_block(128, 128, 64)
    inverse = 1.0 / (agg[256:264, :] + 1e-05)
    inverse_t = inverse.T
    maps = jnp.concatenate([pair_diag(ask), pair_diag(match), pair_diag(content)], axis=1)
    th, tl = split2(agg[0:256, :])
    qkv = dot(jnp.concatenate([th, tl], axis=1), jnp.concatenate([maps, maps], axis=0))

    def spread_out(p, at):
        x = qkv[64 * p : 64 * p + 64, 128 * at : 128 * at + 128]
        x2 = jnp.concatenate([x, x], axis=0)
        return jnp.where(keep, x2, jnp.zeros_like(x2))

    pairs = range(4)
    scores = []
    for p in pairs:
        qh, ql = split2(spread_out(p, 0))
        kh, kl = split2(spread_out(p, 1))
        q3 = jnp.concatenate([qh, ql, qh], axis=1)
        k3 = jnp.concatenate([kh, kh, kl], axis=1)
        scores.append(dot(q3, k3, 1, 1))
    vr = [
        dot(spread_out(p, 2).astype(BF16), res_ref[128 * p : 128 * p + 128, :]).astype(BF16)
        for p in pairs
    ]
    scores = [
        scores[p] * inverse_t[:, p : p + 1] * (inverse[p : p + 1, :] * 0.125) for p in pairs
    ]
    scores = [jnp.where(keep, x, jnp.full_like(x, -1e30)) for x in scores]
    tops = [jnp.max(x, axis=-1, keepdims=True) for x in scores]
    scores = [jnp.exp(scores[p] - tops[p]) for p in pairs]
    sums = [jnp.sum(x, axis=-1, keepdims=True) for x in scores]
    for p in pairs:
        probs = scores[p] * (1.0 / sums[p]) * inverse[p : p + 1, :]
        m_ref[128 * p : 128 * p + 128, :] = dot(probs.astype(BF16), vr[p]).astype(BF16)


def slice_map(part_ref, aff, coef, pt_ref):
    for j in range(2):
        a = aff[4 * j : 4 * j + 4].reshape(256, 64)
        a4 = jnp.concatenate([a, a, a, a], axis=1)
        a4 = jnp.where(same_block(256, 256, 64), a4, jnp.zeros_like(a4))
        both = dot(a4, part_ref[:, 256 * j : 256 * j + 256], 0, 1)
        for i in range(4):
            h = 4 * j + i
            rows = both[64 * i : 64 * i + 64, :] * coef[h]
            pt_ref[64 * h : 64 * h + 64, :] = rows.astype(BF16)


def gelu_twice(x):
    inner = x * (0.7978845608028654 + 0.03567740813636141 * (x * x))
    return x + x * jnp.tanh(inner)


def tile_stages(t, cfg):
    size = cfg["size"]
    at = slice(t * size, t * size + size)
    slabs = range(t * size // SLAB, (t + 1) * size // SLAB)
    live = {}

    def joined(name, rows):
        return jnp.concatenate([cfg[name][i, rows, :] for i in slabs], axis=1)

    def start():
        live["s"] = cfg["s"][at, :].astype(F32)
        if not cfg["first"]:
            live["s"] = live["s"] + dot(joined("w_in", slice(None)), cfg["m"][...], 0, 0)

    def norm():
        live["n"] = layer_norm(live["s"]).astype(BF16)

    def widen():
        live["g"] = gelu_twice(dot(live["n"], cfg["wide"][...])).astype(BF16)

    def contract():
        live["s"] = live["s"] + dot(live["g"], cfg["narrow"][...])

    def finish():
        rows = lax.broadcasted_iota(jnp.int32, (size, 1), 0) + t * size
        s = live["s"]
        cfg["out"][at, :] = jnp.where(rows < cfg["tally"], s, jnp.zeros_like(s)).astype(BF16)
        pltpu.make_async_copy(cfg["out"].at[at], cfg["out_h"].at[at], cfg["sems"].at[t]).start()

    def keep():
        cfg["s_out"][at, :] = live["s"]

    def project():
        live["v"] = dot(live["n"], cfg["val"][...]).astype(BF16)
        live["l"] = dot(cfg["pt"][...], live["n"], 1, 1)

    def weigh():
        cols = lax.broadcasted_iota(jnp.int32, (1, size), 1) + t * size
        on = (cols < cfg["tally"]).astype(F32)
        for h in range(8):
            lg = live["l"][64 * h : 64 * h + 64, :]
            e = jnp.exp2(lg - jnp.max(lg, axis=0, keepdims=True))
            w = e * (on / jnp.sum(e, axis=0, keepdims=True))
            for q, i in enumerate(slabs):
                slab = w[:, SLAB * q : SLAB * q + SLAB]
                cfg["w"][i, 64 * h : 64 * h + 64, :] = slab.astype(BF16)
            part = w[:, 0:128]
            for q in range(1, size // 128):
                part = part + w[:, 128 * q : 128 * q + 128]
            if t == 0:
                cfg["mass"][64 * h : 64 * h + 64, :] = part
            else:
                cfg["mass"][64 * h : 64 * h + 64, :] += part

    def gather():
        for j in range(2):
            part = slice(256 * j, 256 * j + 256)
            y = dot(joined("w", part), live["v"][:, part])
            if t == 0:
                cfg["y"][j] = y
            else:
                cfg["y"][j] += y

    steps = [start]
    if not cfg["first"]:
        steps += [norm, widen, contract]
    if cfg["last"]:
        return steps + [finish]
    if not cfg["first"]:
        steps += [keep]
    return steps + [norm, project, weigh, gather]


def payload(y_ref, mass_ref, pay_ref):
    left = lax.broadcasted_iota(jnp.int32, (64, 128), 1) < 64
    for p in range(4):
        j, q = p // 2, p % 2
        even = y_ref[j, 128 * q : 128 * q + 64, 128 * q : 128 * q + 128]
        odd = y_ref[j, 128 * q + 64 : 128 * q + 128, 128 * q : 128 * q + 128]
        pay_ref[64 * p : 64 * p + 64, :] = jnp.where(left, even, odd)
        row = jnp.sum(mass_ref[128 * p : 128 * p + 128, :].T, axis=0, keepdims=True)
        pay_ref[256 + p : 257 + p, :] = row
    pay_ref[260:PAY_ROWS, :] = jnp.zeros((PAY_ROWS - 260, 128), F32)


def boundary_kernel(layer, first, last, points, *refs):
    refs = list(refs)
    tally_ref = refs.pop(0)
    tally = tally_ref[0]
    size = TILES[0 if first else 2 if last else 1]
    tiles = points // size
    if first:
        sharp_h, x_h, val_h, part_h, aff_h, wide_h, narrow_h = refs[:7]
        sharp_ref, s_ref, aff_ref, wide_ref, narrow_ref, w_ref, pay_ref = refs[7:14]
        val_ref, part_ref, pt_ref, y_ref, mass_ref, sems = refs[14:]
        pairs = [
            (sharp_h, sharp_ref),
            (aff_h, aff_ref),
            (part_h.at[layer], part_ref),
            (x_h, s_ref),
            (val_h.at[layer], val_ref),
            (wide_h, wide_ref),
            (narrow_h, narrow_ref),
        ]
        copies = [pltpu.make_async_copy(a, b, sems.at[i]) for i, (a, b) in enumerate(pairs)]
        for c in copies:
            c.start()
        val_at = part_at = None
        aff_at = layer
    else:
        agg_ref, s_ref, w_in_ref, ask, match, content, res, wide, narrow = refs[:9]
        refs = refs[9:]
        if last:
            out_h, m_ref, half_ref, out_ref, sems = refs
        else:
            sharp_ref, val_ref, part_ref, aff_ref, s_out_ref, w_ref, pay_ref = refs[:7]
            m_ref, half_ref, pt_ref, y_ref, mass_ref = refs[7:]
            val_at = part_at = aff_at = layer
    cfg = dict(size=size, first=first, last=last, tally=tally, s=s_ref)
    if first:
        for c in copies[:3]:
            c.wait()
    if not last:
        coef = [LOG2E / sharp_ref[layer : layer + 1, h : h + 1] for h in range(8)]
        slice_map(part_ref.at[part_at] if part_at is not None else part_ref, aff_ref[aff_at], coef, pt_ref)
        val = val_ref.at[val_at] if val_at is not None else val_ref
        cfg.update(val=val, pt=pt_ref, w=w_ref, y=y_ref, mass=mass_ref)
    if first:
        for c in copies[3:5]:
            c.wait()
    else:
        own = layer - 1
        half_ref[...] = narrow[own] * 0.5
        attend(agg_ref, ask[own], match[own], content[own], res.at[own], m_ref)
        cfg.update(w_in=w_in_ref, m=m_ref, wide=wide.at[own], narrow=half_ref)
        if last:
            cfg.update(out=out_ref, out_h=out_h, sems=sems)
        else:
            cfg.update(s_out=s_out_ref)

    lists = [tile_stages(t, cfg) for t in range(tiles)]
    count = len(lists[0])
    for k in range(count + LAG * (tiles - 1)):
        for t in range(tiles):
            if 0 <= k - LAG * t < count:
                lists[t][k - LAG * t]()
    if last:
        for t in range(tiles):
            at = slice(t * size, t * size + size)
            pltpu.make_async_copy(out_ref.at[at], out_h.at[at], sems.at[t]).wait()
    else:
        payload(y_ref, mass_ref, pay_ref)
    if first:
        for c in copies[5:]:
            c.wait()


def boundary(layer, layers, tally, sharp, agg, s, w, mats):
    first, last = layer == 0, layer == layers
    points, dim = s.shape
    ask, match, content, res, wide, narrow, val, part, aff = mats
    vmem = pl.BlockSpec(memory_space=pltpu.VMEM)
    smem = pl.BlockSpec(memory_space=pltpu.SMEM)
    hbm = pl.BlockSpec(memory_space=pltpu.HBM)
    args, specs = [tally], [smem]
    scratch = []
    sq = (dim, dim)
    sums = [pltpu.VMEM(sq, BF16), pltpu.VMEM((2, 256, 256), F32), pltpu.VMEM((512, 128), F32)]
    if first:
        args += [sharp, s, val, part, aff, wide, narrow]
        specs += [hbm] * 7
        scratch += [pltpu.VMEM(sq, BF16), pltpu.VMEM(sq, BF16)]
        scratch += sums + [pltpu.SemaphoreType.DMA((7,))]
    else:
        args += [agg, s, w, ask, match, content, res, wide, narrow]
        specs += [vmem] * 9
        scratch += [pltpu.VMEM(sq, BF16)] * 2
        if last:
            scratch += [pltpu.VMEM(s.shape, BF16), pltpu.SemaphoreType.DMA((points // TILES[2],))]
        else:
            args += [sharp, val, part, aff]
            specs += [vmem] * 4
            scratch += sums
    if last:
        outs = [jax.ShapeDtypeStruct((points, dim), BF16)]
    else:
        outs = [] if first else [pltpu.VMEM((points, dim), F32)]
        if first:
            outs = [pltpu.VMEM(m.shape, m.dtype) for m in (sharp, s, aff, wide, narrow)]
        outs += [pltpu.VMEM((points // SLAB, dim, SLAB), BF16), pltpu.VMEM((PAY_ROWS, 128), F32)]
    return pl.pallas_call(
        functools.partial(boundary_kernel, layer, first, last, points),
        out_shape=outs,
        in_specs=specs,
        out_specs=[hbm if last else vmem] * len(outs),
        scratch_shapes=scratch,
        compiler_params=pltpu.CompilerParams(vmem_limit_bytes=VMEM_LIMIT),
        name=f"boundary{layer}",
    )(*args)


def fold_kernel(peers, got_ref, out_ref):
    step = PAY_ROWS // peers
    for r in range(step):
        rows = pl.ds(r, peers, stride=step)
        total = jnp.sum(got_ref[rows, :], axis=0, keepdims=True)
        out_ref[rows, :] = jnp.broadcast_to(total, (peers, 128))


def summed(pay):
    peers = lax.axis_size("pts")
    got = lax.all_to_all(pay.reshape(peers, 1, -1), "pts", 0, 0, tiled=True)
    vmem = pl.BlockSpec(memory_space=pltpu.VMEM)
    own = pl.pallas_call(
        functools.partial(fold_kernel, peers),
        out_shape=pltpu.VMEM((PAY_ROWS, 128), F32),
        in_specs=[vmem],
        out_specs=vmem,
        compiler_params=pltpu.CompilerParams(vmem_limit_bytes=2 * 1024 * 1024),
        name="fold",
    )(got.reshape(PAY_ROWS, 128))
    every = lax.all_to_all(own.reshape(peers, 1, -1), "pts", 0, 0, tiled=True)
    return every.reshape(PAY_ROWS, 128)


def per_device(x, tally, val, part, aff, sharp, ask, match, content, res, wide, narrow):
    def placed(space, *arrays):
        return [pltpu.with_memory_space_constraint(a, space) for a in arrays]

    layers = val.shape[0]
    x, sharp, *far = placed(pltpu.HBM, x, sharp, val, part, aff, wide, narrow)
    far = [None] * 4 + [far[3], far[4], *far[:3]]
    sharp, s, aff, wide, narrow, w, pay = boundary(0, layers, tally, sharp, None, x, None, far)
    pay, *later = lax.optimization_barrier((pay, ask, match, content, res, val, part))
    later = placed(pltpu.VMEM, *later)
    near = later[:4] + [wide, narrow] + later[4:] + [aff]
    for layer in range(1, layers + 1):
        got = boundary(layer, layers, tally, sharp, summed(pay), s, w, near)
        if layer < layers:
            s, w, pay = got
    return got[0]


def solution(mesh):
    placed = (P(("batch", "pts"), None), P(("batch", "pts"))) + (P(),) * 10
    return jax.shard_map(
        per_device, mesh=mesh, in_specs=placed, out_specs=P(("batch", "pts"), None), check_vma=False
    )
```
